16 devices in a mesh: col: 2 (over z), row: 8 (over y, x, core).
Axes of the slice: x: 2, y: 2, z: 2, core: 2. Of those that a mesh axis runs over, the one named last changes fastest.
Arguments:
- vel_u: float32 [31, 512, 512], P(None, 'row', 'col')
- vel_v: float32 [31, 512, 512], P(None, 'row', 'col')
- temperature: float32 [31, 512, 512], P(None, 'row', 'col')
- salinity: float32 [31, 512, 512], P(None, 'row', 'col')
- tracers: float32 [31, 10, 512, 512], P(None, None, 'row', 'col')
- surf_eta: float32 [512, 512], P('row', 'col')
- trans_u: float32 [512, 512], P('row', 'col')
- trans_v: float32 [512, 512], P('row', 'col')
- bottom_depth: float32 [512, 512], P('row', 'col')
- level_count: int32 [512, 512], P('row', 'col')
- avg_weights: float32 [30], replicated
Outputs:
- output 1: float32 [512, 512], P('row', 'col')
- output 2: float32 [512, 512], P('row', 'col')
- output 3: float32 [512, 512], P('row', 'col')
- output 4: float32 [31, 512, 512], P(None, 'row', 'col')
- output 5: float32 [31, 512, 512], P(None, 'row', 'col')
- output 6: float32 [31, 512, 512], P(None, 'row', 'col')
- output 7: float32 [31, 512, 512], P(None, 'row', 'col')
- output 8: float32 [31, 10, 512, 512], P(None, None, 'row', 'col')
All inputs are finite; a program needn't handle non-finite values.
Results may differ from the reference program's by a relative error of at most 0.001.
Values sent between devices are 32-bit elements.
A program may use at most 1 GiB of HBM per device.

```python
import jax
import jax.numpy as jnp
from jax import lax

NUM_LEVELS = 31
NUM_SUBCYCLES = 30
NUM_TRACERS = 10
GRID_Y = 512
GRID_X = 512

GRAV_ACC = 400.0
DT_STEP = 0.4
THERMAL_EXP = 0.002
HALINE_CON = 0.004
R_VISC = 2.0
R_DIFF = 0.5


def draw_levels(rng_key):
    key_deep, key_land = jax.random.split(rng_key)
    grid_shape = (GRID_Y, GRID_X)
    levels = jax.random.randint(key_deep, grid_shape, NUM_LEVELS // 2, NUM_LEVELS + 1)
    land_mask = jax.random.randint(key_land, grid_shape, 0, 16) == 0
    levels = jnp.where(land_mask, 0, levels)
    levels = levels.at[0, 0].set(0).at[0, 1].set(NUM_LEVELS)
    return levels.astype(jnp.int32)


def setup_inputs(seed: int = 0) -> dict:
    key_list = jax.random.split(jax.random.key(seed), 11)
    shape_3d = (NUM_LEVELS, GRID_Y, GRID_X)
    shape_2d = (GRID_Y, GRID_X)
    level_frac = ((jnp.arange(NUM_LEVELS, dtype=jnp.float32) + 0.5) / NUM_LEVELS)[:, None, None]
    step_frac = (jnp.arange(NUM_SUBCYCLES, dtype=jnp.float32) + 1.0) / NUM_SUBCYCLES
    raw_weights = step_frac * (1.5 - step_frac) * jax.random.uniform(key_list[10], (NUM_SUBCYCLES,), jnp.float32, 0.2, 1.8)
    return {
        "vel_u": 0.5 * jax.random.normal(key_list[2], shape_3d, jnp.float32),
        "vel_v": 0.5 * jax.random.normal(key_list[3], shape_3d, jnp.float32),
        "temperature": 2.0 * (1.0 - level_frac) + 0.7 * jax.random.normal(key_list[4], shape_3d, jnp.float32),
        "salinity": 0.5 * level_frac + 0.3 * jax.random.normal(key_list[5], shape_3d, jnp.float32),
        "tracers": 1.0 + 0.5 * jax.random.normal(key_list[6], (NUM_LEVELS, NUM_TRACERS, GRID_Y, GRID_X), jnp.float32),
        "surf_eta": 0.05 * jax.random.normal(key_list[7], shape_2d, jnp.float32),
        "trans_u": 0.5 * jax.random.normal(key_list[8], shape_2d, jnp.float32),
        "trans_v": 0.5 * jax.random.normal(key_list[9], shape_2d, jnp.float32),
        "bottom_depth": jax.random.uniform(key_list[1], shape_2d, jnp.float32, 0.3, 1.0),
        "level_count": draw_levels(key_list[0]),
        "avg_weights": raw_weights / jnp.sum(raw_weights),
    }


def shift_east(grid_field):
    return jnp.roll(grid_field, -1, axis=-1)


def shift_west(grid_field):
    return jnp.roll(grid_field, 1, axis=-1)


def shift_north(grid_field):
    return jnp.concatenate([grid_field[..., 1:, :], jnp.zeros_like(grid_field[..., :1, :])], axis=-2)


def shift_south(grid_field):
    return jnp.concatenate([jnp.zeros_like(grid_field[..., :1, :]), grid_field[..., :-1, :]], axis=-2)


def tridiag_coeffs(active, r_coef, num_lev):
    level_idx = jnp.arange(num_lev)[:, None, None]
    sub_diag = jnp.where((level_idx >= 1) & (level_idx < active[None]), -r_coef, 0.0)
    sup_diag = jnp.where(level_idx + 1 < active[None], -r_coef, 0.0)
    return sub_diag, 1.0 - sub_diag - sup_diag, sup_diag


def tridiag_factor(sub_diag, main_diag, sup_diag):
    def elim_step(c_prev, coef_k):
        sub_k, main_k, sup_k = coef_k
        pivot_k = main_k - sub_k * c_prev
        c_new = sup_k / pivot_k
        return c_new, (c_new, pivot_k)
    c_last, factors = lax.scan(elim_step, jnp.zeros_like(main_diag[0]), (sub_diag, main_diag, sup_diag))
    return factors


def tridiag_apply(sub_diag, c_all, pivots, rhs_all):
    def fwd_step(d_prev, xs_k):
        sub_k, pivot_k, rhs_k = xs_k
        d_new = (rhs_k - sub_k * d_prev) / pivot_k
        return d_new, d_new
    d_last, d_all = lax.scan(fwd_step, jnp.zeros_like(rhs_all[0]), (sub_diag, pivots, rhs_all))
    def back_step(x_next, xs_k):
        c_k, d_k = xs_k
        x_new = d_k - c_k * x_next
        return x_new, x_new
    x_first, x_all = lax.scan(back_step, jnp.zeros_like(rhs_all[0]), (c_all, d_all), reverse=True)
    return x_all


def advect_tracer(tracer_field, u_face, v_face):
    flux_x = u_face * jnp.where(u_face > 0, tracer_field, shift_east(tracer_field))
    flux_y = v_face * jnp.where(v_face > 0, tracer_field, shift_north(tracer_field))
    return tracer_field - DT_STEP * ((flux_x - shift_west(flux_x)) + (flux_y - shift_south(flux_y)))


def reference(vel_u, vel_v, temperature, salinity, tracers, surf_eta, trans_u, trans_v, bottom_depth, level_count, avg_weights):
    num_lev = vel_u.shape[0]
    dt_fast = DT_STEP / avg_weights.shape[0]
    level_idx = jnp.arange(num_lev)[:, None, None]
    thick_c = jnp.where(level_count > 0, bottom_depth / jnp.maximum(level_count, 1).astype(jnp.float32), 0.0)
    count_u = jnp.minimum(level_count, shift_east(level_count))
    count_v = jnp.minimum(level_count, shift_north(level_count))
    thick_u = jnp.minimum(thick_c, shift_east(thick_c))
    thick_v = jnp.minimum(thick_c, shift_north(thick_c))
    depth_u = count_u.astype(jnp.float32) * thick_u
    depth_v = count_v.astype(jnp.float32) * thick_v
    mask_c = (level_idx < level_count[None]).astype(jnp.float32)
    mask_u = (level_idx < count_u[None]).astype(jnp.float32)
    mask_v = (level_idx < count_v[None]).astype(jnp.float32)
    wet_c = (level_count > 0).astype(jnp.float32)
    wet_u = (count_u > 0).astype(jnp.float32)
    wet_v = (count_v > 0).astype(jnp.float32)
    u_face = vel_u * mask_u
    v_face = vel_v * mask_v

    density = -THERMAL_EXP * temperature + HALINE_CON * salinity
    pressure = GRAV_ACC * thick_c[None] * (jnp.cumsum(density, axis=0) - 0.5 * density)
    u_east = shift_east(u_face)
    u_west = shift_west(u_face)
    u_north = shift_north(u_face)
    u_south = shift_south(u_face)
    v_east = shift_east(v_face)
    v_west = shift_west(v_face)
    v_north = shift_north(v_face)
    v_south = shift_south(v_face)
    v_at_u = 0.25 * (v_face + v_east + v_south + shift_south(v_east))
    u_at_v = 0.25 * (u_face + u_west + u_north + shift_north(u_west))
    tend_u = (-u_face * 0.5 * (u_east - u_west) - v_at_u * 0.5 * (u_north - u_south) - (shift_east(pressure) - pressure)) * mask_u
    tend_v = (-u_at_v * 0.5 * (v_east - v_west) - v_face * 0.5 * (v_north - v_south) - (shift_north(pressure) - pressure)) * mask_v
    force_u = thick_u * jnp.sum(tend_u, axis=0)
    force_v = thick_v * jnp.sum(tend_v, axis=0)
    sub_u, main_u, sup_u = tridiag_coeffs(count_u, R_VISC, num_lev)
    c_u, pivot_u = tridiag_factor(sub_u, main_u, sup_u)
    pred_u = tridiag_apply(sub_u, c_u, pivot_u, u_face + DT_STEP * tend_u)
    sub_v, main_v, sup_v = tridiag_coeffs(count_v, R_VISC, num_lev)
    c_v, pivot_v = tridiag_factor(sub_v, main_v, sup_v)
    pred_v = tridiag_apply(sub_v, c_v, pivot_v, v_face + DT_STEP * tend_v)

    sub_c, main_c, sup_c = tridiag_coeffs(level_count, R_DIFF, num_lev)
    c_c, pivot_c = tridiag_factor(sub_c, main_c, sup_c)

    def tracer_step(tracer_field):
        advected = advect_tracer(tracer_field, u_face, v_face) * mask_c
        return tridiag_apply(sub_c, c_c, pivot_c, advected) * mask_c

    temp_next = tracer_step(temperature)
    salt_next = tracer_step(salinity)
    tracers_next = jnp.moveaxis(lax.map(tracer_step, jnp.moveaxis(tracers, 1, 0)), 0, 1)

    def subcycle(state_bt, weight):
        eta_c, tu_c, tv_c, avg_u, avg_v = state_bt
        eta_c = (eta_c - dt_fast * ((tu_c - shift_west(tu_c)) + (tv_c - shift_south(tv_c)))) * wet_c
        tu_c = (tu_c + dt_fast * (force_u - GRAV_ACC * depth_u * (shift_east(eta_c) - eta_c))) * wet_u
        tv_c = (tv_c + dt_fast * (force_v - GRAV_ACC * depth_v * (shift_north(eta_c) - eta_c))) * wet_v
        return (eta_c, tu_c, tv_c, avg_u + weight * tu_c, avg_v + weight * tv_c), None

    state_init = (surf_eta * wet_c, trans_u * wet_u, trans_v * wet_v, jnp.zeros_like(trans_u), jnp.zeros_like(trans_v))
    state_final, unused_out = lax.scan(subcycle, state_init, avg_weights)
    eta_next, tu_next, tv_next, avg_u, avg_v = state_final

    safe_u = jnp.where(count_u > 0, depth_u, 1.0)
    safe_v = jnp.where(count_v > 0, depth_v, 1.0)
    levels_u = jnp.maximum(count_u, 1).astype(jnp.float32)
    levels_v = jnp.maximum(count_v, 1).astype(jnp.float32)
    vel_u_next = (pred_u - (jnp.sum(pred_u, axis=0) / levels_u)[None] + (avg_u / safe_u)[None]) * mask_u
    vel_v_next = (pred_v - (jnp.sum(pred_v, axis=0) / levels_v)[None] + (avg_v / safe_v)[None]) * mask_v
    return (eta_next, tu_next, tv_next, vel_u_next, vel_v_next, temp_next, salt_next, tracers_next)
```

```python
import functools

import jax
import jax.numpy as jnp
import numpy as np
from jax import lax
from jax.experimental import pallas as pl
from jax.experimental.pallas import tpu as pltpu
from jax.sharding import PartitionSpec as P

GRAV_ACC = 400.0
DT_STEP = 0.4
THERMAL_EXP = 0.002
HALINE_CON = 0.004
R_VISC = 2.0
R_DIFF = 0.5

LEV = 31
ROWS = 64
LANES = 128
NTR = 10
NSUB = 30
DTB = DT_STEP / NSUB
HALO = 32
BASE = 40
EROWS = 144
PROWS = 80
MESH = pl.DeviceIdType.MESH
F32 = jnp.float32


def pivot_tables(r_coef):
    mid, last = [], []
    prev = None
    for k in range(LEV):
        if k == 0:
            p_mid, p_last = 1.0 + r_coef, 1.0
        else:
            p_mid = 1.0 + 2.0 * r_coef - r_coef * r_coef / prev
            p_last = 1.0 + r_coef - r_coef * r_coef / prev
        mid.append(1.0 / p_mid)
        last.append(1.0 / p_last)
        prev = p_mid
    return mid, last


VISC_MID, VISC_LAST = pivot_tables(R_VISC)
DIFF_MID, DIFF_LAST = pivot_tables(R_DIFF)


def lane_iota(rows):
    return lax.broadcasted_iota(jnp.int32, (rows, LANES), 1)


def inv_pivot(count, k, mid, last):
    kf = float(k)
    return jnp.where(count > kf, jnp.where(count > kf + 1.0, mid[k], last[k]), 0.0)


def momentum_kernel(
    num_col, num_row,
    u_hbm, v_hbm, t_hbm, s_hbm, tr_hbm, eta_hbm, tu_hbm, tv_hbm, bot_hbm, kmt_hbm, w_ref,
    pred_hbm, geo_ref, bt_ref, hn_hbm, hs_hbm, hts_hbm, ew_hbm, uw_hbm, vs_hbm,
    x3, pres, tend, tbuf, ext, comb, geom, kint, cum, force, avg, ews, ewr,
    lsem, tsem, osem, ssem, rsem,
):
    col = lax.axis_index("col")
    row = lax.axis_index("row")
    oth = lax.rem(col + 1, num_col)
    dev_s, dev_n = (col, row - 1), (col, row + 1)
    dev_o, dev_so, dev_no = (oth, row), (oth, row - 1), (oth, row + 1)
    has_s = row > 0
    has_n = row < num_row - 1

    fields2d = (bot_hbm, eta_hbm, tu_hbm, tv_hbm)
    reads2d = []
    for t in range(2):
        lanes = pl.ds(t * LANES, LANES)
        reads2d.append(pltpu.make_async_copy(kmt_hbm.at[:, lanes], kint.at[t], lsem.at[0, t]))
        for i, ref in enumerate(fields2d):
            reads2d.append(
                pltpu.make_async_copy(ref.at[:, lanes], ext.at[1 + i, t, pl.ds(BASE, ROWS), :], lsem.at[1 + i, t])
            )
    reads3d = []
    for f, ref in enumerate((u_hbm, v_hbm, t_hbm, s_hbm)):
        for t in range(2):
            lanes = pl.ds(t * LANES, LANES)
            reads3d.append(
                pltpu.make_async_copy(ref.at[:, :, lanes], x3.at[f, :, t, pl.ds(8, ROWS), :], lsem.at[5 + f, t])
            )
    for cp in reads2d + reads3d:
        cp.start()

    def tracer_read(p):
        return pltpu.make_async_copy(tr_hbm.at[:, pl.ds(2 * p, 2)], tbuf.at[p % 2], tsem.at[p % 2])

    tracer_read(0).start()
    tracer_read(1).start()

    barrier = pltpu.get_barrier_semaphore()
    pl.semaphore_signal(barrier, inc=1, device_id=dev_o, device_id_type=MESH)

    @pl.when(has_s)
    def _():
        pl.semaphore_signal(barrier, inc=1, device_id=dev_s, device_id_type=MESH)
        pl.semaphore_signal(barrier, inc=1, device_id=dev_so, device_id_type=MESH)

    @pl.when(has_n)
    def _():
        pl.semaphore_signal(barrier, inc=1, device_id=dev_n, device_id_type=MESH)
        pl.semaphore_signal(barrier, inc=1, device_id=dev_no, device_id_type=MESH)

    def remote(i, src, dst, dev):
        return pltpu.make_async_remote_copy(
            src_ref=src, dst_ref=dst, send_sem=ssem.at[i], recv_sem=rsem.at[i], device_id=dev, device_id_type=MESH
        )

    lo, hi = pl.ds(BASE, HALO), pl.ds(BASE + ROWS - HALO, HALO)
    above, below = pl.ds(BASE + ROWS, HALO), pl.ds(BASE - HALO, HALO)
    own = pl.ds(BASE, ROWS)

    def plane_copies(first, f0, n):
        fs = pl.ds(f0, n)
        two = pl.ds(0, 2)
        return (
            (remote(first, ext.at[fs, two, lo, :], ext.at[fs, two, above, :], dev_s), "s"),
            (remote(first + 1, ext.at[fs, two, hi, :], ext.at[fs, two, below, :], dev_n), "n"),
            (remote(first + 2, comb.at[fs], ext.at[fs, 2, own, :], dev_o), "o"),
            (remote(first + 3, comb.at[fs, pl.ds(0, HALO), :], ext.at[fs, 2, above, :], dev_so), "s"),
            (remote(first + 4, comb.at[fs, pl.ds(ROWS - HALO, HALO), :], ext.at[fs, 2, below, :], dev_no), "n"),
        )

    def edge_copies(first, f0):
        fs, two = pl.ds(f0, 2), pl.ds(0, 2)
        return (
            (remote(first, x3.at[fs, :, two, pl.ds(8, 1), :], x3.at[fs, :, two, pl.ds(72, 1), :], dev_s), "s"),
            (remote(first + 1, x3.at[fs, :, two, pl.ds(71, 1), :], x3.at[fs, :, two, pl.ds(7, 1), :], dev_n), "n"),
        )

    geo_copies = plane_copies(0, 0, 2)
    state_copies = plane_copies(5, 2, 3)
    force_copies = plane_copies(10, 5, 2)
    uv_copies = edge_copies(15, 0) + (
        (remote(17, x3.at[0, :, 1, pl.ds(8, 1), :], x3.at[0, :, 2, pl.ds(72, 1), :], dev_so), "s"),
        (remote(18, x3.at[1, :, 0, pl.ds(71, 1), :], x3.at[1, :, 2, pl.ds(7, 1), :], dev_no), "n"),
    )
    ts_copies = edge_copies(19, 2)
    ew_copies = [((remote(21, ews.at[0], ewr.at[0], dev_o), "o"),), ((remote(22, ews.at[1], ewr.at[1], dev_o), "o"),)]
    for p in range(NTR // 2):
        ew_copies.append(((remote(23 + p, ews.at[2 + p], ew_hbm.at[1 + p], dev_o), "o"),))
    tr_copies = (
        (remote(28, tr_hbm.at[:, :, pl.ds(0, 1), :], hn_hbm, dev_s), "s"),
        (remote(29, tr_hbm.at[:, :, pl.ds(ROWS - 1, 1), :], hs_hbm, dev_n), "n"),
    )

    def run_by_side(copies, action, receiving):
        for side, cond in (("o", None), ("s", has_n if receiving else has_s), ("n", has_s if receiving else has_n)):
            picked = [cp for cp, s in copies if s == side]
            if not picked:
                continue
            if cond is None:
                for cp in picked:
                    action(cp)
            else:

                @pl.when(cond)
                def _(picked=picked):
                    for cp in picked:
                        action(cp)

    def start(copies):
        run_by_side(copies, lambda cp: cp.start(), False)

    def wait_recv(copies):
        run_by_side(copies, lambda cp: cp.wait_recv(), True)

    def wait_send(copies):
        run_by_side(copies, lambda cp: cp.wait_send(), False)

    def zero_wall(rows2d, row3d):
        for f in range(7):
            for t in range(3):
                ext[f, t, rows2d, :] = jnp.zeros((HALO, LANES), F32)

        def body(k, carry):
            for f in range(4):
                for t in range(3):
                    x3[f, k, t, pl.ds(row3d, 1), :] = jnp.zeros((1, LANES), F32)
            return carry

        lax.fori_loop(0, LEV, body, 0)

    @pl.when(jnp.logical_not(has_s))
    def _():
        zero_wall(below, 7)

    @pl.when(jnp.logical_not(has_n))
    def _():
        zero_wall(above, 72)

    for cp in reads2d:
        cp.wait()
    half = lane_iota(ROWS) < LANES // 2
    for t in range(2):
        ext[0, t, own, :] = kint[t].astype(F32)
    for f in range(5):
        comb[f] = jnp.where(half, ext[f, 0, own, :], ext[f, 1, own, :])

    pl.semaphore_wait(barrier, 1 + 2 * has_s.astype(jnp.int32) + 2 * has_n.astype(jnp.int32))

    for cp in reads3d[:4]:
        cp.wait()
    start(uv_copies)
    start(geo_copies)

    lane = lane_iota(ROWS)
    slab_of_lane = lane // 2

    def pack(group, load):
        acc = jnp.zeros((ROWS, LANES), F32)
        for f in range(2):

            def body(k, acc, f=f):
                slab = k + f * LEV
                left, right = load(f, k)
                edge = pltpu.roll(jnp.where(half, left, right), 2 * slab + 1, 1)
                return jnp.where(slab_of_lane == slab, edge, acc)

            acc = lax.fori_loop(0, LEV, body, acc)
        ews[group] = acc

    rows3 = pl.ds(8, ROWS)
    pack(0, lambda f, k: (x3[f, k, 0, rows3, :], x3[f, k, 1, rows3, :]))
    for cp in reads3d[4:]:
        cp.wait()
    start(ew_copies[0])
    start(ts_copies)
    pack(1, lambda f, k: (x3[2 + f, k, 0, rows3, :], x3[2 + f, k, 1, rows3, :]))
    start(state_copies)
    for p in range(NTR // 2):
        tracer_read(p).wait()
        start(ew_copies[1 + p])
        if p == 0:
            start(tr_copies)
        slot = p % 2
        pack(
            2 + p,
            lambda f, k: (tbuf[slot, k, f, :, pl.ds(0, LANES)], tbuf[slot, k, f, :, pl.ds(LANES, LANES)]),
        )
        if p + 2 < NTR // 2:
            tracer_read(p + 2).start()

    wait_recv(geo_copies)
    start(ew_copies[1 + NTR // 2])
    chunk = 32
    first_lane, last_lane = lane_iota(chunk) == 0, lane_iota(chunk) == LANES - 1

    def east(tiles, n=3):
        rolled = [pltpu.roll(x, LANES - 1, 1) for x in tiles]
        edge = last_lane if tiles[0].shape[0] == chunk else lane_iota(tiles[0].shape[0]) == LANES - 1
        return [jnp.where(edge, rolled[(t + 1) % 3], rolled[t]) for t in range(n)]

    def west(tiles, n=3):
        rolled = [pltpu.roll(x, 1, 1) for x in tiles]
        edge = first_lane if tiles[0].shape[0] == chunk else lane_iota(tiles[0].shape[0]) == 0
        return [jnp.where(edge, rolled[(t + 2) % 3], rolled[t]) for t in range(n)]

    def thickness(count, bottom):
        return jnp.where(count > 0.0, bottom / jnp.maximum(count, 1.0), 0.0)

    for c in range(8, 8 + ROWS + 2 * HALO, chunk):
        rs, rn = pl.ds(c, chunk), pl.ds(c + 1, chunk)
        kc = [ext[0, t, rs, :] for t in range(3)]
        hc = [thickness(kc[t], ext[1, t, rs, :]) for t in range(3)]
        kn = [ext[0, t, rn, :] for t in range(3)]
        hn = [thickness(kn[t], ext[1, t, rn, :]) for t in range(3)]
        ke, he = east(kc), east(hc)
        for t in range(3):
            ku, kv = jnp.minimum(kc[t], ke[t]), jnp.minimum(kc[t], kn[t])
            geom[0, t, rs, :] = ku
            geom[1, t, rs, :] = kv
            geom[2, t, rs, :] = (DTB * DTB * GRAV_ACC) * (ku * jnp.minimum(hc[t], he[t]))
            geom[3, t, rs, :] = (DTB * DTB * GRAV_ACC) * (kv * jnp.minimum(hc[t], hn[t]))
            geom[4, t, rs, :] = jnp.where(kc[t] > 0.0, 1.0, 0.0)
            geom[5, t, rs, :] = GRAV_ACC * hc[t]

    wait_send(uv_copies)
    wait_recv(uv_copies)
    wait_recv(ts_copies)
    wait_recv(ew_copies[0])
    wait_recv(ew_copies[1])
    for t in range(3):
        cum[t] = jnp.zeros((PROWS, LANES), F32)
    gr = BASE - 8

    def mask_level(k, carry):
        kf = k.astype(F32)
        for f in range(2):
            for t in range(2):
                x3[f, k, t] = jnp.where(kf < geom[f, t, pl.ds(gr, PROWS), :], x3[f, k, t], 0.0)
            edge = pltpu.roll(ewr[0], 2 * LANES - 1 - 2 * (k + f * LEV), 1)
            x3[f, k, 2, rows3, :] = jnp.where(kf < geom[f, 2, own, :], edge, 0.0)
            corner = 72 if f == 0 else 0
            x3[f, k, 2, pl.ds(corner, 8), :] = jnp.where(
                kf < geom[f, 2, pl.ds(gr + corner, 8), :], x3[f, k, 2, pl.ds(corner, 8), :], 0.0
            )
        for t in range(3):
            rs = pl.ds(8, 72) if t < 2 else rows3
            if t < 2:
                tt, ss = x3[2, k, t, rs, :], x3[3, k, t, rs, :]
            else:
                tt = pltpu.roll(ewr[1], 2 * LANES - 1 - 2 * k, 1)
                ss = pltpu.roll(ewr[1], 2 * LANES - 1 - 2 * (k + LEV), 1)
            rho = HALINE_CON * ss - THERMAL_EXP * tt
            total = cum[t, rs, :] + rho
            cum[t, rs, :] = total
            pres[k, t, rs, :] = geom[5, t, pl.ds(BASE, rs.size), :] * (total - 0.5 * rho)
        return carry

    lax.fori_loop(0, LEV, mask_level, 0)

    outs = [
        pltpu.make_async_copy(x3.at[0, :, 2, rows3, :], uw_hbm, osem.at[0]),
        pltpu.make_async_copy(x3.at[1, :, pl.ds(0, 2), pl.ds(7, 1), :], vs_hbm, osem.at[1]),
        pltpu.make_async_copy(x3.at[pl.ds(2, 2), :, pl.ds(0, 2), pl.ds(72, 1), :], hts_hbm.at[0], osem.at[2]),
        pltpu.make_async_copy(x3.at[pl.ds(2, 2), :, pl.ds(0, 2), pl.ds(7, 1), :], hts_hbm.at[1], osem.at[3]),
        pltpu.make_async_copy(ewr.at[1], ew_hbm.at[0], osem.at[4]),
    ]
    for cp in outs:
        cp.start()

    for f in range(2):
        for t in range(2):
            force[f, t] = jnp.zeros((ROWS, LANES), F32)

    def tend_level(k, carry):
        kf = k.astype(F32)
        for c in range(0, ROWS, chunk):
            rs, rn, rb = pl.ds(8 + c, chunk), pl.ds(9 + c, chunk), pl.ds(7 + c, chunk)
            uc = [x3[0, k, t, rs, :] for t in range(3)]
            vc = [x3[1, k, t, rs, :] for t in range(3)]
            un = [x3[0, k, t, rn, :] for t in range(3)]
            vb = [x3[1, k, t, rb, :] for t in range(3)]
            pc = [pres[k, t, rs, :] for t in range(3)]
            ue, uw, ve, vw = east(uc, 2), west(uc, 2), east(vc, 2), west(vc, 2)
            unw, vbe, pe = west(un, 2), east(vb, 2), east(pc, 2)
            for t in range(2):
                ub = x3[0, k, t, rb, :]
                vn = x3[1, k, t, rn, :]
                pn = pres[k, t, rn, :]
                va = (vc[t] + ve[t]) + (vb[t] + vbe[t])
                ua = (uc[t] + uw[t]) + (un[t] + unw[t])
                gu = -0.5 * (uc[t] * (ue[t] - uw[t])) - 0.125 * (va * (un[t] - ub)) - (pe[t] - pc[t])
                gv = -0.125 * (ua * (ve[t] - vw[t])) - 0.5 * (vc[t] * (vn - vb[t])) - (pn - pc[t])
                gs = pl.ds(BASE + c, chunk)
                gu = jnp.where(kf < geom[0, t, gs, :], gu, 0.0)
                gv = jnp.where(kf < geom[1, t, gs, :], gv, 0.0)
                cs = pl.ds(c, chunk)
                tend[0, k, t, cs, :] = uc[t] + DT_STEP * gu
                tend[1, k, t, cs, :] = vc[t] + DT_STEP * gv
                force[0, t, cs, :] += gu
                force[1, t, cs, :] += gv
        return carry

    lax.fori_loop(0, LEV, tend_level, 0)

    def face_thickness(c):
        rs, rn = pl.ds(BASE + c, chunk), pl.ds(BASE + c + 1, chunk)
        hc = [thickness(ext[0, t, rs, :], ext[1, t, rs, :]) for t in range(3)]
        he = east(hc, 2)
        hn = [thickness(ext[0, t, rn, :], ext[1, t, rn, :]) for t in range(2)]
        return [jnp.minimum(hc[t], he[t]) for t in range(2)], [jnp.minimum(hc[t], hn[t]) for t in range(2)]

    for c in range(0, ROWS, chunk):
        hu, hv = face_thickness(c)
        cs = pl.ds(c, chunk)
        for f, hf in ((0, hu), (1, hv)):
            scaled = [(DTB * DTB) * (hf[t] * force[f, t, cs, :]) for t in range(2)]
            for t in range(2):
                ext[5 + f, t, pl.ds(BASE + c, chunk), :] = scaled[t]
            comb[5 + f, cs, :] = jnp.where(lane_iota(chunk) < LANES // 2, scaled[0], scaled[1])

    wait_recv(state_copies)
    wait_send(state_copies)
    for c in range(8, 8 + ROWS + 2 * HALO, chunk):
        rs = pl.ds(c, chunk)
        for t in range(3):
            ext[2, t, rs, :] = ext[2, t, rs, :] * geom[4, t, rs, :]
            for f in range(2):
                ext[3 + f, t, rs, :] = jnp.where(geom[f, t, rs, :] > 0.0, DTB * ext[3 + f, t, rs, :], 0.0)
    start(force_copies)

    def solve_rows(b, carry):
        r0 = pl.multiple_of(b * 8, 8)
        rs = pl.ds(r0, 8)
        count = [[geom[f, t, pl.ds(pl.multiple_of(BASE + b * 8, 8), 8), :] for t in range(2)] for f in range(2)]
        prev = [[jnp.zeros((8, LANES), F32)] * 2 for f in range(2)]
        for k in range(LEV):
            for f in range(2):
                for t in range(2):
                    inv = inv_pivot(count[f][t], k, VISC_MID, VISC_LAST)
                    rhs = tend[f, k, t, rs, :]
                    prev[f][t] = (rhs + R_VISC * prev[f][t]) * inv if k else rhs * inv
                    tend[f, k, t, rs, :] = prev[f][t]
        total = [[prev[f][t] for t in range(2)] for f in range(2)]
        for k in range(LEV - 2, -1, -1):
            for f in range(2):
                for t in range(2):
                    prev[f][t] = tend[f, k, t, rs, :] + (R_VISC * VISC_MID[k]) * prev[f][t]
                    total[f][t] = total[f][t] + prev[f][t]
                    tend[f, k, t, rs, :] = prev[f][t]
        for f in range(2):
            for t in range(2):
                force[f, t, rs, :] = total[f][t] / jnp.maximum(count[f][t], 1.0)
        return carry

    lax.fori_loop(0, ROWS // 8, solve_rows, 0)
    pred_out = pltpu.make_async_copy(tend, pred_hbm, osem.at[5])
    pred_out.start()

    for f in range(2):
        for t in range(2):
            avg[f, t] = jnp.zeros((ROWS, LANES), F32)
    wait_recv(force_copies)

    def subcycle(n, carry):
        wn = w_ref[n]
        for c in range(8, 8 + ROWS + 2 * HALO, chunk):
            rs, rb = pl.ds(c, chunk), pl.ds(c - 1, chunk)
            uc = [ext[3, t, rs, :] for t in range(3)]
            uw = west(uc)
            for t in range(3):
                div = (uc[t] - uw[t]) + (ext[4, t, rs, :] - ext[4, t, rb, :])
                ext[2, t, rs, :] = (ext[2, t, rs, :] - div) * geom[4, t, rs, :]
        for c in range(8, 8 + ROWS + 2 * HALO, chunk):
            rs, rn = pl.ds(c, chunk), pl.ds(c + 1, chunk)
            ec = [ext[2, t, rs, :] for t in range(3)]
            ee = east(ec)
            for t in range(3):
                un = ext[3, t, rs, :] + (ext[5, t, rs, :] - geom[2, t, rs, :] * (ee[t] - ec[t]))
                vn = ext[4, t, rs, :] + (ext[6, t, rs, :] - geom[3, t, rs, :] * (ext[2, t, rn, :] - ec[t]))
                ext[3, t, rs, :] = un
                ext[4, t, rs, :] = vn
                if t < 2 and BASE <= c < BASE + ROWS:
                    cs = pl.ds(c - BASE, chunk)
                    avg[0, t, cs, :] += wn * un
                    avg[1, t, cs, :] += wn * vn
        return carry

    wait_send(force_copies)
    lax.fori_loop(0, NSUB, subcycle, 0)

    for c in range(0, ROWS, chunk):
        hu, hv = face_thickness(c)
        rs, cs = pl.ds(BASE + c, chunk), pl.ds(c, chunk)
        for t in range(2):
            ku, kv = geom[0, t, rs, :], geom[1, t, rs, :]
            geo_ref[0, t, cs, :] = ext[0, t, rs, :]
            geo_ref[1, t, cs, :] = ku
            geo_ref[2, t, cs, :] = kv
            for f, kf, hf in ((0, ku, hu), (1, kv, hv)):
                safe = jnp.where(kf > 0.0, kf * hf[t], 1.0)
                geo_ref[3 + f, t, cs, :] = (avg[f, t, cs, :] * (1.0 / DTB)) / safe - force[f, t, cs, :]
            bt_ref[0, t, cs, :] = ext[2, t, rs, :]
            bt_ref[1, t, cs, :] = ext[3, t, rs, :] * (1.0 / DTB)
            bt_ref[2, t, cs, :] = ext[4, t, rs, :] * (1.0 / DTB)

    for cp in outs:
        cp.wait()
    pred_out.wait()
    wait_send(geo_copies)
    wait_send(ts_copies)
    for g, copies in enumerate(ew_copies):
        if g >= 2:
            wait_recv(copies)
        wait_send(copies)
    wait_recv(tr_copies)
    wait_send(tr_copies)


def tracer_kernel(
    num_row,
    u_hbm, v_hbm, t_hbm, s_hbm, tr_hbm, pred_hbm, geo_ref, bt_ref, hn_hbm, hs_hbm, hts_hbm, ew_ref, uw_ref, vs_hbm,
    eta_out, tu_out, tv_out, un_hbm, vn_hbm, tn_hbm, sn_hbm, trn_hbm,
    qbuf, dbuf, coef,
    isem, hsem, osem,
):
    row = lax.axis_index("row")
    has_s = row > 0
    has_n = row < num_row - 1
    own = pl.ds(8, ROWS)
    npair = 1 + NTR // 2

    def block_reads(p):
        slot = p % 2
        cps = []
        for f in range(2):
            for t in range(2):
                lanes = pl.ds(t * LANES, LANES)
                if p == 0:
                    src = (t_hbm, s_hbm)[f].at[:, :, lanes]
                elif p < npair:
                    src = tr_hbm.at[:, 2 * (p - 1) + f, :, lanes]
                else:
                    src = pred_hbm.at[f, :, t]
                cps.append(pltpu.make_async_copy(src, qbuf.at[slot, f, :, t, own, :], isem.at[slot, f, t]))
        return cps

    def halo_reads(p):
        slot = p % 2
        north, south = [], []
        if p >= npair:
            return north, south
        for f in range(2):
            for t in range(2):
                lanes = pl.ds(t * LANES, LANES)
                if p == 0:
                    sn, ss = hts_hbm.at[0, f, :, t], hts_hbm.at[1, f, :, t]
                else:
                    q = 2 * (p - 1) + f
                    sn, ss = hn_hbm.at[:, q, :, lanes], hs_hbm.at[:, q, :, lanes]
                north.append(pltpu.make_async_copy(sn, qbuf.at[slot, f, :, t, pl.ds(72, 1), :], hsem.at[slot, 0, f, t]))
                south.append(pltpu.make_async_copy(ss, qbuf.at[slot, f, :, t, pl.ds(7, 1), :], hsem.at[slot, 1, f, t]))
        return north, south

    def for_all(p, action):
        for cp in block_reads(p):
            action(cp)
        north, south = halo_reads(p)
        if north:

            @pl.when(has_n)
            def _():
                for cp in north:
                    action(cp)

            @pl.when(has_s)
            def _():
                for cp in south:
                    action(cp)

    def out_copies(p):
        slot = p % 2
        cps = []
        for f in range(2):
            for t in range(2):
                lanes = pl.ds(t * LANES, LANES)
                if p == 0:
                    dst = (tn_hbm, sn_hbm)[f].at[:, :, lanes]
                elif p < npair:
                    dst = trn_hbm.at[:, 2 * (p - 1) + f, :, lanes]
                else:
                    dst = (un_hbm, vn_hbm)[f].at[:, :, lanes]
                cps.append(pltpu.make_async_copy(dbuf.at[slot, f, :, t], dst, osem.at[slot, f, t]))
        return cps

    vel = []
    for f, ref in enumerate((u_hbm, v_hbm)):
        for t in range(2):
            vel.append(
                pltpu.make_async_copy(
                    ref.at[:, :, pl.ds(t * LANES, LANES)], qbuf.at[1, f, :, t, own, :], isem.at[1, f, t]
                )
            )
    for t in range(2):
        vel.append(pltpu.make_async_copy(vs_hbm.at[:, t], qbuf.at[1, 1, :, t, pl.ds(7, 1), :], hsem.at[1, 1, 1, t]))
    for cp in vel:
        cp.start()

    def zero_rows(r):
        def body(k, carry):
            for f in range(2):
                for t in range(2):
                    qbuf[0, f, k, t, pl.ds(r, 1), :] = jnp.zeros((1, LANES), F32)
            return carry

        lax.fori_loop(0, LEV, body, 0)

    @pl.when(jnp.logical_not(has_s))
    def _():
        zero_rows(7)

    @pl.when(jnp.logical_not(has_n))
    def _():
        zero_rows(72)

    for_all(0, lambda cp: cp.start())
    for t in range(2):
        lanes = pl.ds(t * LANES, LANES)
        for i, ref in enumerate((eta_out, tu_out, tv_out)):
            ref[:, lanes] = bt_ref[i, t]
    first_lane, last_lane = lane_iota(8) == 0, lane_iota(8) == LANES - 1
    for cp in vel:
        cp.wait()

    def coef_rows(b, carry):
        r0 = pl.multiple_of(b * 8, 8)
        rs = pl.ds(r0, 8)
        km = [geo_ref[0, t, rs, :] for t in range(2)]
        ku = [geo_ref[1, t, rs, :] for t in range(2)]
        kv = [geo_ref[2, t, rs, :] for t in range(2)]
        for k in range(LEV):
            kf = float(k)
            um = [jnp.where(ku[t] > kf, qbuf[1, 0, k, t, pl.ds(r0 + 8, 8), :], 0.0) for t in range(2)]
            rolled = [pltpu.roll(x, 1, 1) for x in um]
            edge = pltpu.roll(uw_ref[k, rs, :], 1, 1)
            uw = [jnp.where(first_lane, edge, rolled[0]), jnp.where(first_lane, rolled[0], rolled[1])]
            for t in range(2):
                inv = inv_pivot(km[t], k, DIFF_MID, DIFF_LAST)
                dti = DT_STEP * inv
                vm = jnp.where(kv[t] > kf, qbuf[1, 1, k, t, pl.ds(r0 + 8, 8), :], 0.0)
                vs = coef[5, k, t, rs, :]
                ue_in, uw_in = jnp.minimum(um[t], 0.0), jnp.maximum(uw[t], 0.0)
                vn_in, vs_in = jnp.minimum(vm, 0.0), jnp.maximum(vs, 0.0)
                out = (jnp.maximum(um[t], 0.0) - jnp.minimum(uw[t], 0.0)) + (
                    jnp.maximum(vm, 0.0) - jnp.minimum(vs, 0.0)
                )
                coef[0, k, t, rs, :] = inv - dti * out
                coef[1, k, t, rs, :] = -dti * ue_in
                coef[2, k, t, rs, :] = dti * uw_in
                coef[3, k, t, rs, :] = -dti * vn_in
                coef[4, k, t, rs, :] = dti * vs_in
                coef[5, k, t, rs, :] = R_DIFF * inv
        return carry

    def south_level(k, carry):
        kf = k.astype(F32)
        for t in range(2):
            v0 = qbuf[1, 1, k, t, own, :]
            qbuf[1, 1, k, t, own, :] = jnp.where(geo_ref[2, t] > kf, v0, 0.0)
            coef[5, k, t] = qbuf[1, 1, k, t, pl.ds(7, ROWS), :]
        return carry

    lax.fori_loop(0, LEV, south_level, 0)
    lax.fori_loop(0, ROWS // 8, coef_rows, 0)

    def wall_rows_again():
        def body_at(r):
            def body(k, carry):
                for f in range(2):
                    for t in range(2):
                        qbuf[1, f, k, t, pl.ds(r, 1), :] = jnp.zeros((1, LANES), F32)
                return carry

            lax.fori_loop(0, LEV, body, 0)

        @pl.when(jnp.logical_not(has_s))
        def _():
            body_at(7)

        @pl.when(jnp.logical_not(has_n))
        def _():
            body_at(72)

    wall_rows_again()

    for p in range(npair + 1):
        slot = p % 2
        for_all(p, lambda cp: cp.wait())
        if p < npair:
            for_all(p + 1, lambda cp: cp.start())
        if p >= 2:
            for cp in out_copies(p - 2):
                cp.wait()

        if p < npair:

            def pair_rows(b, carry, p=p, slot=slot):
                r0 = pl.multiple_of(b * 8, 8)
                rs = pl.ds(r0, 8)
                ew = ew_ref[p, rs, :]
                prev = [[None, None], [None, None]]
                for k in range(LEV):
                    cf = [[coef[i, k, t, rs, :] for t in range(2)] for i in range(6)]
                    for f in range(2):
                        s = k + f * LEV
                        q = [qbuf[slot, f, k, t, pl.ds(r0 + 8, 8), :] for t in range(2)]
                        qn = [qbuf[slot, f, k, t, pl.ds(r0 + 9, 8), :] for t in range(2)]
                        qs = [qbuf[slot, f, k, t, pl.ds(r0 + 7, 8), :] for t in range(2)]
                        he = pltpu.roll(ew, (2 * LANES - 2 - 2 * s) % LANES, 1)
                        hw = pltpu.roll(ew, (LANES - 2 * s) % LANES, 1) if s else ew
                        re = [pltpu.roll(x, LANES - 1, 1) for x in q]
                        rw = [pltpu.roll(x, 1, 1) for x in q]
                        qe = [jnp.where(last_lane, re[1], re[0]), jnp.where(last_lane, he, re[1])]
                        qw = [jnp.where(first_lane, hw, rw[0]), jnp.where(first_lane, rw[0], rw[1])]
                        for t in range(2):
                            d = (
                                (cf[0][t] * q[t] + cf[1][t] * qe[t])
                                + (cf[2][t] * qw[t] + cf[3][t] * qn[t])
                                + cf[4][t] * qs[t]
                            )
                            if k:
                                d = d + cf[5][t] * prev[f][t]
                            prev[f][t] = d
                            dbuf[slot, f, k, t, rs, :] = d
                for k in range(LEV - 2, -1, -1):
                    for f in range(2):
                        for t in range(2):
                            prev[f][t] = dbuf[slot, f, k, t, rs, :] + (R_DIFF * DIFF_MID[k]) * prev[f][t]
                            dbuf[slot, f, k, t, rs, :] = prev[f][t]
                return carry

            lax.fori_loop(0, ROWS // 8, pair_rows, 0)
        else:

            def correct_level(k, carry, slot=slot):
                kf = k.astype(F32)
                for f in range(2):
                    for t in range(2):
                        dbuf[slot, f, k, t] = jnp.where(
                            geo_ref[1 + f, t] > kf, qbuf[slot, f, k, t, own, :] + geo_ref[3 + f, t], 0.0
                        )
                return carry

            lax.fori_loop(0, LEV, correct_level, 0)
        for cp in out_copies(p):
            cp.start()
    for p in (npair - 1, npair):
        for cp in out_copies(p):
            cp.wait()


def solution(mesh):
    num_col = mesh.shape["col"]
    num_row = mesh.shape["row"]
    hbm = pl.BlockSpec(memory_space=pltpu.HBM)
    vmem = pl.BlockSpec(memory_space=pltpu.VMEM)

    def sds(*shape):
        return jax.ShapeDtypeStruct(shape, F32)

    def local_step(vel_u, vel_v, temperature, salinity, tracers, surf_eta, trans_u, trans_v, bottom, levels, weights):
        wide = 2 * LANES
        mid = pl.pallas_call(
            functools.partial(momentum_kernel, num_col, num_row),
            out_shape=(
                sds(2, LEV, 2, ROWS, LANES),
                sds(5, 2, ROWS, LANES),
                sds(3, 2, ROWS, LANES),
                sds(LEV, NTR, 1, wide),
                sds(LEV, NTR, 1, wide),
                sds(2, 2, LEV, 2, 1, LANES),
                sds(1 + NTR // 2, ROWS, LANES),
                sds(LEV, ROWS, LANES),
                sds(LEV, 2, 1, LANES),
            ),
            in_specs=[hbm] * 10 + [pl.BlockSpec(memory_space=pltpu.SMEM)],
            out_specs=(hbm, vmem, vmem, hbm, hbm, hbm, hbm, hbm, hbm),
            scratch_shapes=[
                pltpu.VMEM((4, LEV, 3, PROWS, LANES), F32),
                pltpu.VMEM((LEV, 3, PROWS, LANES), F32),
                pltpu.VMEM((2, LEV, 2, ROWS, LANES), F32),
                pltpu.VMEM((2, LEV, 2, ROWS, wide), F32),
                pltpu.VMEM((7, 3, EROWS, LANES), F32),
                pltpu.VMEM((7, ROWS, LANES), F32),
                pltpu.VMEM((6, 3, EROWS, LANES), F32),
                pltpu.VMEM((2, ROWS, LANES), jnp.int32),
                pltpu.VMEM((3, PROWS, LANES), F32),
                pltpu.VMEM((2, 2, ROWS, LANES), F32),
                pltpu.VMEM((2, 2, ROWS, LANES), F32),
                pltpu.VMEM((2 + NTR // 2, ROWS, LANES), F32),
                pltpu.VMEM((2, ROWS, LANES), F32),
                pltpu.SemaphoreType.DMA((9, 2)),
                pltpu.SemaphoreType.DMA((2,)),
                pltpu.SemaphoreType.DMA((6,)),
                pltpu.SemaphoreType.DMA((30,)),
                pltpu.SemaphoreType.DMA((30,)),
            ],
            compiler_params=pltpu.CompilerParams(
                collective_id=0, has_side_effects=True, vmem_limit_bytes=56 * 2**20
            ),
            name="momentum",
        )(vel_u, vel_v, temperature, salinity, tracers, surf_eta, trans_u, trans_v, bottom, levels, weights)
        pred, geo, bt, hn, hs, hts, ew, uw, vs = mid
        return pl.pallas_call(
            functools.partial(tracer_kernel, num_row),
            out_shape=(
                sds(ROWS, wide), sds(ROWS, wide), sds(ROWS, wide),
                sds(LEV, ROWS, wide), sds(LEV, ROWS, wide), sds(LEV, ROWS, wide), sds(LEV, ROWS, wide),
                sds(LEV, NTR, ROWS, wide),
            ),
            in_specs=[hbm] * 6 + [vmem, vmem, hbm, hbm, hbm, vmem, vmem, hbm],
            out_specs=(vmem,) * 3 + (hbm,) * 5,
            scratch_shapes=[
                pltpu.VMEM((2, 2, LEV, 2, PROWS, LANES), F32),
                pltpu.VMEM((2, 2, LEV, 2, ROWS, LANES), F32),
                pltpu.VMEM((6, LEV, 2, ROWS, LANES), F32),
                pltpu.SemaphoreType.DMA((2, 2, 2)),
                pltpu.SemaphoreType.DMA((2, 2, 2, 2)),
                pltpu.SemaphoreType.DMA((2, 2, 2)),
            ],
            compiler_params=pltpu.CompilerParams(vmem_limit_bytes=56 * 2**20),
            name="tracers",
        )(vel_u, vel_v, temperature, salinity, tracers, pred, geo, bt, hn, hs, hts, ew, uw, vs)

    spec_3d = P(None, "row", "col")
    spec_4d = P(None, None, "row", "col")
    spec_2d = P("row", "col")
    in_specs = (spec_3d, spec_3d, spec_3d, spec_3d, spec_4d, spec_2d, spec_2d, spec_2d, spec_2d, spec_2d, P())
    out_specs = (spec_2d, spec_2d, spec_2d, spec_3d, spec_3d, spec_3d, spec_3d, spec_4d)
    return jax.shard_map(local_step, mesh=mesh, in_specs=in_specs, out_specs=out_specs, check_vma=False)
```
